128 devices in a mesh: ep: 32 (over z, x, core), dp: 4 (over y).
Axes of the slice: x: 4, y: 4, z: 4, core: 2. Of those that a mesh axis runs over, the one named last changes fastest.
Arguments:
- grad_out: float32 [16384, 1536], P(('ep', 'dp')), may hold values from -6 to 6
- tokens: bfloat16 [16384, 1536], P(('ep', 'dp')), may hold values from -6 to 6
- probs: float32 [16384, 4], P(('ep', 'dp')), may hold values from 0.1 to 0.5
- expert_ids: int32 [16384, 4], P(('ep', 'dp')), may hold values from 0 to 31, all different within a row; in each aligned block of 128 rows (0 to 127, 128 to 255, ...) at most 20 rows name the same one
- priority: int32 [128, 128], P(('ep', 'dp')), may hold values from 0 to 127, each once within a row
- cap_counts: int32 [32], replicated, may hold values from 10 to 20, as said below
- gate_weight: bfloat16 [32, 1536, 1536], P('ep'), may hold values from -0.15625 to 0.15625
- up_weight: bfloat16 [32, 1536, 1536], P('ep'), may hold values from -0.15625 to 0.15625
- down_weight: bfloat16 [32, 1536, 1536], P('ep'), may hold values from -0.15625 to 0.15625
Outputs:
- input_grad: bfloat16 [16384, 1536], P(('ep', 'dp'))
- prob_grad: float32 [16384, 4], P(('ep', 'dp'))
- gate_grad: bfloat16 [32, 1536, 1536], P('ep', 'dp')
- up_grad: bfloat16 [32, 1536, 1536], P('ep', 'dp')
- down_grad: bfloat16 [32, 1536, 1536], P('ep', 'dp')
The draws below stay inside these ranges and needn't reach their ends.
Inputs may be any that keep to these rules, and one draw needn't show every extreme that they name: `expert_ids`: each row names 4 different experts; among the rows of one device no expert is named by more than 20 rows, and in some device some expert is named by exactly 20 rows. `priority`: each row orders the 128 tokens of one device, each number once. `cap_counts`: some expert has exactly 20.
All inputs are finite; a program needn't handle non-finite values. Where the reference program divides by a largest or mean magnitude, that divisor is 1e-20 or more.
Results may differ from the reference program's by a relative error of at most 0.017.
Values may be sent and summed in bfloat16 or wider, within the bound.
A program may use at most 128 MiB of HBM per device.

```python
import math
import jax
import jax.numpy as jnp
import numpy as np
from jax import lax

D = 1536
FH = 1536
TOP = 4
TOK_DEV = 128
EXPERTS = 32
TOKENS = 16384
CAP = 20
N_EP = 32
N_DP = 4


def draw_cap_counts(key, part):
    first_key, second_key = jax.random.split(jax.random.fold_in(key, 17))
    counts = jax.random.randint(first_key, (EXPERTS,), CAP // 2, CAP + 1)
    chosen = jax.random.randint(second_key, (), 0, EXPERTS)
    return jnp.where(jnp.arange(EXPERTS) == chosen, CAP, counts).astype(jnp.int32)


def level_of(own_key, dims, shards, smallest, largest):
    level, own = 1.0, jax.random.fold_in(own_key, 6)
    for dim, shards_of in shards:
        draws = jnp.exp(jax.random.uniform(jax.random.fold_in(own, dim), (shards_of,), jnp.float32, smallest / len(shards), largest / len(shards)))
        level = level * jnp.repeat(draws, dims[dim] // shards_of).reshape([-1 if axis == dim else 1 for axis in range(len(dims))])
    return level


def deal_out(rng, own, number, rows, amount, top, bound, slope):
    order = jax.random.permutation(rng, amount)
    crowded, common = load_shares(amount, rows * top, bound, slope, True), load_shares(amount, rows * top, bound, slope, False)
    places = jnp.arange(amount)

    def named(tallies, rotation):
        used = int((tallies > 0).sum())
        fixed = max(1, used // 4)
        passed = fixed + (places - fixed + rotation * (used - fixed)) % max(1, amount - fixed)
        return jnp.zeros((amount,), jnp.int32).at[order[jnp.where(places < fixed, places, passed)]].set(jnp.asarray(tallies, jnp.int32))

    tallies = jnp.where(number % 4 == 0, named(crowded, number // 4), named(common, number - number // 4 - 1))
    mixed = jax.random.permutation(jax.random.fold_in(own, 3), amount)
    source_of, sink = mixed[0:amount // 2 * 2:2], mixed[1:amount // 2 * 2:2]
    room = jnp.minimum(tallies[source_of] - 1, bound - tallies[sink]) // 2
    room = jnp.where((source_of == order[0]) | (sink == order[0]) | (tallies[sink] == 0), 0, jnp.maximum(room, 0))
    passed = jax.random.randint(jax.random.fold_in(own, 4), (amount // 2,), 0, 1 << 20) % (room + 1)
    tallies = tallies.at[source_of].add(-passed).at[sink].add(passed)
    members = jnp.searchsorted(jnp.cumsum(tallies), jnp.arange(rows * top), side="right").astype(jnp.int32)
    table = members.reshape(top, rows).T
    table = table[jax.random.permutation(jax.random.fold_in(own, 1), rows)]
    rotation = jax.random.randint(jax.random.fold_in(own, 2), (rows, 1), 0, top)
    return jnp.take_along_axis(table, (jnp.arange(top)[None, :] + rotation) % top, axis=1)


def load_shares(amount, total, bound, slope, full):
    loads = [(1 << 20) // math.isqrt(rank ** slope) + 1 for rank in range(1, amount + 1)]
    largest = bound if full else min(bound, max(-(-total // amount), total * loads[0] // sum(loads)))
    least = 1 if total - largest >= amount - 1 else 0
    given, surplus = [largest] + [least] * (amount - 1), total - largest - least * (amount - 1)
    while surplus > 0:
        candidates = [i for i in range(1, amount) if given[i] < largest] or [i for i in range(1, amount) if given[i] < bound]
        whole, budget = sum([loads[i] for i in candidates]), surplus
        for i in candidates:
            addition = min(bound - given[i], max(1, budget * loads[i] // whole), surplus)
            given[i] = given[i] + addition
            surplus = surplus - addition
    return np.array(given)


def gaussian(own_key, extent, scale, reach, cuts=(), kind=jnp.bfloat16):
    loudness = level_of(own_key, extent, cuts, -0.22, 0.18) if cuts else 1.0
    entries = jax.random.normal(own_key, extent, jnp.float32) * scale * loudness
    return jnp.minimum(jnp.maximum(entries, -reach), reach).astype(kind)


def setup_inputs(seed: int = 0) -> dict:
    key_of = jax.random.split(jax.random.key(seed), 10)
    grad_out = gaussian(key_of[0], (TOKENS, D), 1.0, 6.0, ((0, 128),), jnp.float32)
    tokens = gaussian(key_of[1], (TOKENS, D), 1.0, 6.0, ((0, 128),))
    probs = jnp.clip(0.1 + 0.4 * jax.random.uniform(key_of[2], (TOKENS, TOP), jnp.float32) ** level_of(key_of[2], (TOKENS, TOP), ((0, 128),), -0.2, 0.2), 0.1, 0.5)
    expert_ids_keys = jax.random.split(jax.random.fold_in(key_of[3], 1), TOKENS // TOK_DEV)
    expert_ids_turns = jax.random.permutation(jax.random.fold_in(key_of[3], 3), TOKENS // TOK_DEV)
    expert_ids = jax.vmap(lambda own, number: deal_out(jax.random.fold_in(key_of[3], 2), own, number, TOK_DEV, EXPERTS, TOP, CAP, 2))(expert_ids_keys, expert_ids_turns).reshape((TOKENS, TOP))
    priority = jax.vmap(lambda own: jax.random.permutation(own, TOK_DEV))(jax.random.split(key_of[4], (N_EP * N_DP))).reshape((N_EP * N_DP, TOK_DEV)).astype(jnp.int32)
    cap_counts = draw_cap_counts(jax.random.fold_in(key_of[9], 71), 0)
    gate_weight = gaussian(key_of[6], (EXPERTS, FH, D), D ** -0.5, 0.15625, ((0, 32),))
    up_weight = gaussian(key_of[7], (EXPERTS, FH, D), D ** -0.5, 0.15625, ((0, 32),))
    down_weight = gaussian(key_of[8], (EXPERTS, FH, D), D ** -0.5, 0.15625, ((0, 32),))
    return dict(grad_out=grad_out, tokens=tokens, probs=probs, expert_ids=expert_ids, priority=priority, cap_counts=cap_counts, gate_weight=gate_weight, up_weight=up_weight, down_weight=down_weight)


sharpness = 1.702


def contract_last(first_op, second_op):
    return lax.dot_general(first_op, second_op, (((1,), (1,)), ((), ())), preferred_element_type=jnp.float32)


def replica_sum(deltas, values):
    per_replica = N_EP * CAP
    partials = jnp.einsum("rsf,rsd->rfd", deltas.reshape(N_DP, per_replica, FH).astype(jnp.float32), values.reshape(N_DP, per_replica, D).astype(jnp.float32), precision=lax.Precision.HIGHEST)
    rounded = lax.optimization_barrier(partials.astype(jnp.bfloat16))
    return jnp.sum(rounded.astype(jnp.float32), axis=0).astype(jnp.bfloat16)


def reference(grad_out, tokens, probs, expert_ids, priority, cap_counts, gate_weight, up_weight, down_weight):
    blocks = N_EP * N_DP
    slot_rows = N_EP * CAP
    total_slots = N_DP * slot_rows
    block_ids = expert_ids.reshape(blocks, TOK_DEV, TOP)
    expert_range = jnp.arange(EXPERTS, dtype=jnp.int32)
    routed = jnp.any(block_ids[:, :, :, None] == expert_range, axis=2).astype(jnp.float32)
    earlier = (priority[:, None, :] < priority[:, :, None]).astype(jnp.float32)
    before = jnp.einsum("bsu,bue->bse", earlier, routed, precision=lax.Precision.HIGHEST)
    slot_rank = jnp.take_along_axis(before, block_ids, axis=2).astype(jnp.int32)
    kept = slot_rank < cap_counts[block_ids]
    block_range = jnp.arange(blocks, dtype=jnp.int32)
    source = block_range // N_DP
    replica = block_range % N_DP
    position = (replica[:, None, None] * slot_rows + source[:, None, None] * CAP + slot_rank).reshape(TOKENS, TOP)
    kept = kept.reshape(TOKENS, TOP)
    row_scale = jnp.maximum(jnp.max(jnp.abs(grad_out), axis=1), 1.0)
    quantized = (grad_out / row_scale[:, None]).astype(jnp.bfloat16)

    def one_expert(running, inputs):
        input_acc, prob_acc = running
        expert, w_gate, w_up, w_down = inputs
        live_pair = kept & (expert_ids == expert)
        target = jnp.where(live_pair, position, total_slots).astype(jnp.int32)
        input_buf = jnp.zeros((total_slots + 1, D), jnp.bfloat16)
        grad_buf = jnp.zeros((total_slots + 1, D), jnp.bfloat16)
        scale_buf = jnp.zeros((total_slots + 1,), jnp.float32)
        prob_buf = jnp.zeros((total_slots + 1,), jnp.float32)
        for which in range(TOP):
            input_buf = input_buf.at[target[:, which]].set(tokens)
            grad_buf = grad_buf.at[target[:, which]].set(quantized)
            scale_buf = scale_buf.at[target[:, which]].set(row_scale)
            prob_buf = prob_buf.at[target[:, which]].set(probs[:, which])
        slot_x = input_buf[:total_slots]
        slot_q = grad_buf[:total_slots]
        slot_scale = scale_buf[:total_slots]
        slot_prob = prob_buf[:total_slots]
        gate_pre = contract_last(slot_x, w_gate)
        up_pre = contract_last(slot_x, w_up)
        back_proj = contract_last(slot_q, w_down)
        squash = jax.nn.sigmoid(sharpness * gate_pre)
        gated = gate_pre * squash
        activated = (up_pre + 1.0) * gated
        weight = (slot_scale * slot_prob)[:, None]
        act_delta = weight * back_proj
        up_delta = (act_delta * gated).astype(jnp.bfloat16)
        gate_delta = (act_delta * (up_pre + 1.0) * (squash + sharpness * gate_pre * squash * (1.0 - squash))).astype(jnp.bfloat16)
        act_scaled = (activated * weight).astype(jnp.bfloat16)
        slot_in = (jnp.dot(gate_delta, w_gate, preferred_element_type=jnp.float32) + jnp.dot(up_delta, w_up, preferred_element_type=jnp.float32)).astype(jnp.bfloat16)
        slot_pgrad = slot_scale * jnp.sum(activated * back_proj, axis=1)
        pad_in = jnp.concatenate([slot_in, jnp.zeros((1, D), jnp.bfloat16)], axis=0)
        pad_prob = jnp.concatenate([slot_pgrad, jnp.zeros((1,), jnp.float32)], axis=0)
        for which in range(TOP):
            input_acc = input_acc + pad_in[target[:, which]].astype(jnp.float32)
        prob_acc = prob_acc + pad_prob[target]
        grads = (replica_sum(gate_delta, slot_x), replica_sum(up_delta, slot_x), replica_sum(act_scaled, slot_q))
        return (input_acc, prob_acc), grads

    start = (jnp.zeros((TOKENS, D), jnp.float32), jnp.zeros((TOKENS, TOP), jnp.float32))
    (input_acc, prob_acc), grads = lax.scan(one_expert, start, (expert_range, gate_weight, up_weight, down_weight))
    return input_acc.astype(jnp.bfloat16), prob_acc, grads[0], grads[1], grads[2]
```

```python
import jax
import jax.numpy as jnp
from jax import lax
from jax.sharding import PartitionSpec as P

sharpness = 1.702


def contract_last(first_op, second_op):
    return lax.dot_general(
        first_op, second_op, (((1,), (1,)), ((), ())), preferred_element_type=jnp.float32
    )


def contract_first(first_op, second_op):
    return lax.dot_general(
        first_op, second_op, (((0,), (0,)), ((), ())), preferred_element_type=jnp.float32
    )


def route_table(expert_ids, priority, cap_counts, buckets, capacity):
    ranking = priority[0]
    earlier = (ranking[None, :] < ranking[:, None]).astype(jnp.float32)
    expert_range = lax.broadcasted_iota(jnp.int32, (1, 1, buckets), 2)
    matches = (expert_ids[:, :, None] == expert_range).astype(jnp.float32)
    routed = jnp.sum(matches, axis=1)
    before = jnp.dot(earlier, routed)
    slot_rank = jnp.sum(matches * before[:, None, :], axis=2)
    keep_limit = jnp.sum(matches * cap_counts.astype(jnp.float32)[None, None, :], axis=2)
    slot_range = lax.broadcasted_iota(jnp.float32, (1, 1, capacity), 2)
    slot_hit = (
        (slot_rank[:, :, None] == slot_range) & (slot_rank < keep_limit)[:, :, None]
    ).astype(jnp.float32)
    placement = matches[:, :, :, None] * slot_hit[:, :, None, :]
    return placement.reshape(expert_ids.shape[0], expert_ids.shape[1], buckets * capacity)


def deltas(slot_x, slot_g, w_gate, w_up, w_down):
    gate_pre = contract_last(slot_x, w_gate)
    up_pre = contract_last(slot_x, w_up)
    act_delta = contract_last(slot_g, w_down)
    squash = jax.nn.sigmoid(sharpness * gate_pre)
    gated = gate_pre * squash
    activated = (up_pre + 1.0) * gated
    up_delta = (act_delta * gated).astype(jnp.bfloat16)
    gate_delta = (
        act_delta * (up_pre + 1.0) * (squash + sharpness * gate_pre * squash * (1.0 - squash))
    ).astype(jnp.bfloat16)
    return activated, act_delta, gate_delta, up_delta


def on_device(
    grad_out, tokens, probs, expert_ids, priority, cap_counts, gate_weight, up_weight, down_weight
):
    ep_size = lax.axis_size("ep")
    dp_size = lax.axis_size("dp")
    tok_rows, model_width = tokens.shape
    route_count = expert_ids.shape[1]
    capacity = 5 * route_count * tok_rows // (4 * ep_size)
    slot_rows = ep_size * capacity
    placement = route_table(expert_ids, priority, cap_counts, ep_size, capacity)
    slot_table = jnp.sum(placement, axis=1)
    table_low = slot_table.astype(jnp.bfloat16)
    row_scale = jnp.maximum(jnp.max(jnp.abs(grad_out), axis=1), 1.0)
    quantized = (grad_out / row_scale[:, None]).astype(jnp.bfloat16)
    send_prob = jnp.sum(placement * probs[:, :, None], axis=(0, 1))
    send_scale = jnp.sum(slot_table * row_scale[:, None], axis=0)
    send_x = jnp.einsum("ts,td->sd", table_low, tokens, preferred_element_type=jnp.float32).astype(
        jnp.bfloat16
    )
    send_g = (
        jnp.einsum("ts,td->sd", table_low, quantized, preferred_element_type=jnp.float32)
        * (send_prob * send_scale)[:, None]
    ).astype(jnp.bfloat16)
    bucket_shape = (ep_size, capacity, model_width)

    def exchange(a):
        return lax.all_to_all(a, "ep", split_axis=0, concat_axis=0, tiled=True)

    slot_x = exchange(send_x.reshape(bucket_shape)).reshape(slot_rows, model_width)
    all_x = lax.all_gather(slot_x, "dp", axis=0, tiled=True)
    slot_g = exchange(send_g.reshape(bucket_shape)).reshape(slot_rows, model_width)
    all_g = lax.all_gather(slot_g, "dp", axis=0, tiled=True)
    w_gate = gate_weight[0]
    w_up = up_weight[0]
    w_down = down_weight[0]
    activated, act_delta, gate_delta, up_delta = deltas(slot_x, slot_g, w_gate, w_up, w_down)
    slot_in = (
        jnp.dot(gate_delta, w_gate, preferred_element_type=jnp.float32)
        + jnp.dot(up_delta, w_up, preferred_element_type=jnp.float32)
    ).astype(jnp.bfloat16)
    slot_out = jnp.sum(activated * act_delta, axis=1)
    back_in = exchange(slot_in.reshape(bucket_shape))
    back_prob = exchange(slot_out.reshape(ep_size, capacity).astype(jnp.bfloat16))
    prob_grad = jnp.einsum("tks,s->tk", placement, back_prob.reshape(slot_rows)) / probs
    input_grad = jnp.einsum(
        "ts,sd->td",
        table_low,
        back_in.reshape(slot_rows, model_width),
        preferred_element_type=jnp.float32,
    ).astype(jnp.bfloat16)
    share = w_gate.shape[0] // dp_size
    first = lax.axis_index("dp") * share

    def mine(w):
        return lax.dynamic_slice_in_dim(w, first, share, 0)

    act_mine, _, gd_mine, ud_mine = deltas(all_x, all_g, mine(w_gate), mine(w_up), mine(w_down))
    gate_share = contract_first(gd_mine, all_x).astype(jnp.bfloat16)
    up_share = contract_first(ud_mine, all_x).astype(jnp.bfloat16)
    down_share = contract_first(act_mine.astype(jnp.bfloat16), all_g).astype(jnp.bfloat16)
    return (input_grad, prob_grad, gate_share[None], up_share[None], down_share[None])


def solution(mesh):
    return jax.shard_map(
        on_device,
        mesh=mesh,
        in_specs=(
            P(("ep", "dp"), None),
            P(("ep", "dp"), None),
            P(("ep", "dp"), None),
            P(("ep", "dp"), None),
            P(("ep", "dp"), None),
            P(),
            P("ep", None, None),
            P("ep", None, None),
            P("ep", None, None),
        ),
        out_specs=(
            P(("ep", "dp"), None),
            P(("ep", "dp"), None),
            P("ep", "dp", None),
            P("ep", "dp", None),
            P("ep", "dp", None),
        ),
        check_vma=False,
    )
```
